256 devices in a mesh: expert: 16 (over z_lo, x), shard: 16 (over z_hi, y, core).
Axes of the slice: x: 4, y: 4, z: 8 (z_hi: 2, z_lo: 4; z = z_hi * 4 + z_lo), core: 2. Of those that a mesh axis runs over, the one named last changes fastest.
Arguments:
- train_down: float32 [16, 6400, 4096], P('expert', None, 'shard'), may hold values from -0.109375 to 0.109375
- router_weight: float32 [4096, 16], P('shard', 'expert'), may hold values from -0.09375 to 0.09375
- router_gain: float32 [4096], P('shard'), may hold values from 0.25 to 1.75
Outputs:
- ready_down: bfloat16 [16, 6400, 4096], P('expert', 'shard')
- scale_down: float32 [16, 6400], P('expert', 'shard')
- serve_router: bfloat16 [4096, 16], replicated
The draws below stay inside these ranges and needn't reach their ends.
All inputs are finite; a program needn't handle non-finite values. Where the reference program divides by a largest or mean magnitude, that divisor is 1e-20 or more.
Results may differ from the reference program's by a relative error of at most 0.001.
Values may be sent and summed in bfloat16 or wider, within the bound.
A program may use at most 64 MiB of HBM per device.

```python
import jax
import jax.numpy as jnp

EXPERTS = 16
D_MODEL = 4096
D_EXPERT = 6400


def raised(drawn, rng, source, target, parts, factor):
    def block_of(position):
        return (jnp.arange(drawn.shape[position]) // (drawn.shape[position] // parts)).reshape((-1,) + (1,) * (drawn.ndim - 1 - position))

    first = jax.random.permutation(rng, parts)[block_of(target)]
    other_side = (block_of(target) + parts // 2) % parts
    return jnp.where((block_of(source) == first) | (block_of(source) == other_side), factor * drawn, drawn)


def level_of(rng, shape, pieces, least, high):
    factor_of, own = 1.0, jax.random.fold_in(rng, 6)
    for dim, parts in pieces:
        heights = jnp.exp(jax.random.uniform(jax.random.fold_in(own, dim), (parts,), jnp.float32, least / len(pieces), high / len(pieces)))
        factor_of = factor_of * jnp.repeat(heights, shape[dim] // parts).reshape([-1 if axis == dim else 1 for axis in range(len(shape))])
    return factor_of


def normal_values(key, shape, width, bound, split=(), held_as=jnp.bfloat16):
    result = width * jax.random.normal(key, shape, jnp.float32)
    if split:
        result = result * level_of(key, shape, split, -0.22, 0.18)
    return jnp.clip(result, -bound, bound).astype(held_as)


def noise_with(key, dims, spread, most, cuts, heavy, kind=jnp.bfloat16):
    result = spread * jax.random.normal(key, dims, jnp.float32)
    if cuts:
        result = result * level_of(key, dims, cuts, -0.22, 0.18)
    return jnp.clip(raised(result, jax.random.fold_in(key, 3), *heavy), -most, most).astype(kind)


def setup_inputs(seed: int = 0) -> dict:
    streams_of = jax.random.split(jax.random.key(seed), 4)
    train_down = noise_with(streams_of[0], (EXPERTS, D_EXPERT, D_MODEL), D_EXPERT ** -0.5, 0.109375, ((0, 16), (2, 16)), (2, 1, 16, 2.0), jnp.float32)
    router_weight = normal_values(streams_of[1], (D_MODEL, EXPERTS), D_MODEL ** -0.5, 0.09375, ((0, 16), (1, 16)), jnp.float32)
    router_gain = jnp.clip(1.0 + 0.15 * jax.random.normal(streams_of[2], (D_MODEL,), jnp.float32), 0.25, 1.75)
    return dict(train_down=train_down, router_weight=router_weight, router_gain=router_gain)


def reference(train_down, router_weight, router_gain):
    scale_down = jnp.max(jnp.abs(train_down), axis=2)
    ready_down = (train_down / jnp.expand_dims(scale_down, 2)).astype(jnp.bfloat16)
    serve_router = (router_weight * router_gain[:, None]).astype(jnp.bfloat16)
    return ready_down, scale_down, serve_router
```

```python
import jax
import jax.numpy as jnp
from jax import lax
from jax.experimental import pallas as pl
from jax.experimental.pallas import tpu as pltpu
from jax.sharding import PartitionSpec as P

MESH = pl.DeviceIdType.MESH
PEERS = 16
ROWS, COLS = 400, 256
GROUPS = ROWS // 8
RAW = 16
EARLY = 64
FIRST = RAW + EARLY
REST = ROWS - FIRST
FAR = [(1, dy, dc) for dy in (2, 1, 3, 0) for dc in (0, 1)]
NEAR = [(0, dy, dc) for dy in (2, 1, 3, 0) for dc in (0, 1) if (dy, dc) != (0, 0)]
OFFSETS = FAR + NEAR
BACK = [OFFSETS.index((dz, -dy % 4, dc)) for dz, dy, dc in OFFSETS]


def kernel(
    x_ref, w_ref, g_ref, o_ref, sc_ref, rt_ref,
    xbuf, send, raw, early_mine, early_all, part_mine, part_all, full_all, wbuf, rb,
    load_sem, in_sem,
    early_s, early_r, part_s, part_r, raw_s, raw_r, full_s, full_r,
    da_s, da_r, db_s, db_r, z_s, z_r, xy_s, xy_r, co_s, co_r,
):
    e, s = lax.axis_index("expert"), lax.axis_index("shard")
    zl, xx = e // 4, e % 4
    zh, yy, cc = s // 8, (s // 2) % 4, s % 2
    zz = zh * 4 + zl

    def partner(k):
        dz, dy, dc = OFFSETS[k]
        return ((zh + dz) % 2) * 8 + ((yy + dy) % 4) * 2 + (cc + dc) % 2

    def on_line(k):
        z = (zz + k) % 8
        return {"expert": (z % 4) * 4 + xx, "shard": (z // 4) * 8 + yy * 2 + cc}

    def on_plane(k):
        x, y = (xx + k // 4) % 4, (yy + k % 4) % 4
        return {"expert": zl * 4 + x, "shard": zh * 8 + y * 2 + cc}

    order = [partner(k) for k in range(PEERS - 1)] + [s]
    loads = []
    for k, d in enumerate(order):
        c = pltpu.make_async_copy(x_ref.at[pl.ds(d * ROWS, ROWS)], xbuf.at[d], load_sem.at[k])
        c.start()
        loads.append(c)
    small = [
        pltpu.make_async_copy(w_ref, wbuf.at[0], in_sem.at[0]),
        pltpu.make_async_copy(g_ref, wbuf.at[1], in_sem.at[1]),
    ]
    for c in small:
        c.start()

    barrier = pltpu.get_barrier_semaphore()
    greeted = 0
    for k in range(PEERS - 1):
        pl.semaphore_signal(barrier, inc=1, device_id={"shard": partner(k)}, device_id_type=MESH)
        greeted += 1
    for k in range(1, 8):
        if k != 4:
            pl.semaphore_signal(barrier, inc=1, device_id=on_line(k), device_id_type=MESH)
            greeted += 1
    for k in range(1, 16):
        if k // 4:
            pl.semaphore_signal(barrier, inc=1, device_id=on_plane(k), device_id_type=MESH)
            greeted += 1

    for c in small:
        c.wait()
    rb[xx, yy, cc, zz] = (wbuf[0] * wbuf[1]).astype(jnp.bfloat16).astype(jnp.float32)

    lane = lax.broadcasted_iota(jnp.int32, (8, 128), 1)
    for c in loads:
        c.wait()

    def maxima(d, early):
        part = jnp.zeros((8, 128), jnp.float32)
        for g in range(GROUPS):
            v = jnp.abs(xbuf[d, 8 * g : 8 * g + 8, :])
            top = jnp.max(jnp.maximum(v[:, :128], v[:, 128:]), axis=1, keepdims=True)
            part = jnp.where(lane == g, top, part)
            if RAW <= 8 * g < FIRST:
                early = jnp.where(lane == d * (EARLY // 8) + g - RAW // 8, top, early)
        part_mine[d] = part
        return early

    early_mine[...] = lax.fori_loop(0, PEERS, maxima, jnp.zeros((8, 128), jnp.float32))
    early_all[s] = early_mine[...]
    part_all[s] = part_mine[s]

    pl.semaphore_wait(barrier, greeted)

    def remote(src, dst, ss, rs, device):
        c = pltpu.make_async_remote_copy(
            src_ref=src, dst_ref=dst, send_sem=ss, recv_sem=rs, device_id=device, device_id_type=MESH
        )
        c.start()
        return c

    pending = []
    early, part, rawc, full, da, db = [], [], [], [], [], []
    for k in range(PEERS - 1):
        early.append(remote(early_mine, early_all.at[s], early_s.at[k], early_r.at[k], {"shard": partner(k)}))
    for k in range(PEERS - 1):
        d = partner(k)
        part.append(remote(part_mine.at[d], part_all.at[s], part_s.at[k], part_r.at[k], {"shard": d}))
    line = [
        remote(rb.at[xx, yy, cc, zz], rb.at[xx, yy, cc, zz], z_s.at[k], z_r.at[k], on_line(k)) for k in range(1, 8)
    ]
    for k in range(PEERS - 1):
        d = partner(k)
        rawc.append(remote(xbuf.at[d, pl.ds(0, RAW)], raw.at[s], raw_s.at[k], raw_r.at[k], {"shard": d}))

    for c in part:
        c.wait_recv()
    mine = jnp.max(part_all[...], axis=0)
    full_all[s] = mine
    for c in early:
        c.wait_recv()
    inverse_early = 1.0 / jnp.max(early_all[...], axis=0)
    for k in range(PEERS - 1):
        full.append(remote(full_all.at[s], full_all.at[s], full_s.at[k], full_r.at[k], {"shard": partner(k)}))

    mine_safe = jnp.where(lane < GROUPS, mine, 1.0)
    inverse_mine = 1.0 / mine_safe

    def early_rows(d):
        for j in range(EARLY // 16):
            tops = []
            for h in range(2):
                at = d * (EARLY // 8) + 2 * j + h
                tops.append(jnp.sum(jnp.where(lane == at, inverse_early, 0.0), axis=1, keepdims=True))
            lo = RAW + 16 * j
            send[d, lo : lo + 16, :] = (xbuf[d, lo : lo + 16, :] * jnp.concatenate(tops, axis=0)).astype(jnp.bfloat16)

    columns = pl.ds(pl.multiple_of(s * COLS, COLS), COLS)

    def send_early(k):
        d = partner(k)
        da.append(
            remote(
                send.at[d, pl.ds(RAW, EARLY)], o_ref.at[pl.ds(RAW, EARLY), columns],
                da_s.at[k], da_r.at[k], {"shard": d},
            )
        )

    for k in range(PEERS - 1):
        early_rows(partner(k))
        if k:
            send_early(k - 1)
    send_early(PEERS - 2)

    def rest_rows(d):
        inverse = 1.0 / jnp.where(lane < GROUPS, full_all[d], 1.0)
        for j in range(FIRST // 16, ROWS // 16):
            tops = jnp.concatenate([inverse[:, 2 * j : 2 * j + 1], inverse[:, 2 * j + 1 : 2 * j + 2]], axis=0)
            send[d, 16 * j : 16 * j + 16, :] = (xbuf[d, 16 * j : 16 * j + 16, :] * tops).astype(jnp.bfloat16)

    def send_rest(k):
        d = partner(k)
        db.append(
            remote(
                send.at[d, pl.ds(FIRST, REST)], o_ref.at[pl.ds(FIRST, REST), columns],
                db_s.at[k], db_r.at[k], {"shard": d},
            )
        )

    for k in range(PEERS - 1):
        full[BACK[k]].wait_recv()
        rest_rows(partner(k))
        if k:
            send_rest(k - 1)
    send_rest(PEERS - 2)

    for c in line:
        c.wait_recv()
    plane = [
        remote(rb.at[xx, yy, cc], rb.at[xx, yy, cc], xy_s.at[k], xy_r.at[k], on_plane(k)) for k in range(1, 16)
    ]

    for j in range(ROWS // 16):
        tops = jnp.concatenate([inverse_mine[:, 2 * j : 2 * j + 1], inverse_mine[:, 2 * j + 1 : 2 * j + 2]], axis=0)
        o_ref[16 * j : 16 * j + 16, columns] = (xbuf[s, 16 * j : 16 * j + 16, :] * tops).astype(jnp.bfloat16)
    for c in rawc:
        c.wait_recv()
    for k in range(PEERS - 1):
        d = partner(k)
        for j in range(RAW // 16):
            tops = jnp.concatenate([inverse_mine[:, 2 * j : 2 * j + 1], inverse_mine[:, 2 * j + 1 : 2 * j + 2]], axis=0)
            o_ref[16 * j : 16 * j + 16, pl.ds(pl.multiple_of(d * COLS, COLS), COLS)] = (
                raw[d, 16 * j : 16 * j + 16, :] * tops
            ).astype(jnp.bfloat16)

    sub = lax.broadcasted_iota(jnp.int32, (8, 128), 0)
    for b in range(pl.cdiv(ROWS, 128)):
        row = jnp.zeros((8, 128), jnp.float32)
        for g in range(16 * b, min(16 * b + 16, GROUPS)):
            here = (lane // 8 == g - 16 * b) & (sub == lane % 8)
            row = jnp.where(here, jnp.broadcast_to(mine[:, g : g + 1], (8, 128)), row)
        width = min(128, ROWS - 128 * b)
        sc_ref[:, 128 * b : 128 * b + width] = jnp.max(row, axis=0, keepdims=True)[:, :width]

    for c in plane:
        c.wait_recv()
    other = remote(
        rb.at[:, :, cc], rb.at[:, :, cc], co_s.at[0], co_r.at[0],
        {"shard": zh * 8 + yy * 2 + 1 - cc},
    )
    other.wait_recv()

    def router_columns(t, carry):
        h, y, c = t // 8, (t // 2) % 4, t % 2
        rows = [rb[r % 4, y, c, h * 4 + r // 4] for r in range(16)]
        rt_ref[:, pl.ds(pl.multiple_of(t * COLS, COLS), COLS)] = jnp.concatenate(rows, axis=0).astype(jnp.bfloat16)
        return carry

    lax.fori_loop(0, PEERS, router_columns, 0)

    for c in da + db:
        c.wait_recv()
    for c in early + part + line + rawc + full + da + db + plane + [other]:
        c.wait_send()


def per_device(train_down, router_weight, router_gain):
    x = train_down[0]
    w = router_weight.reshape(1, COLS)
    g = router_gain.reshape(1, COLS)
    f32, bf16 = jnp.float32, jnp.bfloat16
    dma = pltpu.SemaphoreType.DMA
    pairs = lambda n: [dma((n,)), dma((n,))]
    n = PEERS - 1
    hbm = pl.BlockSpec(memory_space=pltpu.HBM)
    vmem = pl.BlockSpec(memory_space=pltpu.VMEM)
    o, sc, rt = pl.pallas_call(
        kernel,
        out_shape=(
            pltpu.VMEM((ROWS, PEERS * COLS), bf16),
            pltpu.VMEM((1, ROWS), f32),
            pltpu.VMEM((PEERS, PEERS * COLS), bf16),
        ),
        in_specs=[hbm] * 3,
        out_specs=(vmem,) * 3,
        scratch_shapes=[
            pltpu.VMEM((PEERS, ROWS, COLS), f32),
            pltpu.VMEM((PEERS, ROWS, COLS), bf16),
            pltpu.VMEM((PEERS, RAW, COLS), f32),
            pltpu.VMEM((8, 128), f32),
            pltpu.VMEM((PEERS, 8, 128), f32),
            pltpu.VMEM((PEERS, 8, 128), f32),
            pltpu.VMEM((PEERS, 8, 128), f32),
            pltpu.VMEM((PEERS, 8, 128), f32),
            pltpu.VMEM((2, 1, COLS), f32),
            pltpu.VMEM((4, 4, 2, 8, 1, COLS), f32),
            dma((PEERS,)), dma((2,)),
            *pairs(n), *pairs(n), *pairs(n), *pairs(n), *pairs(n), *pairs(n),
            *pairs(8), *pairs(16), *pairs(1),
        ],
        compiler_params=pltpu.CompilerParams(
            collective_id=0, has_side_effects=True, vmem_limit_bytes=40 * 2**20
        ),
        name="exchange",
    )(x, w, g)
    return o[None], sc, rt.T


def solution(mesh):
    in_specs = (P("expert", None, "shard"), P("shard", "expert"), P("shard"))
    out_specs = (P("expert", "shard", None), P("expert", "shard"), P())
    return jax.shard_map(per_device, mesh=mesh, in_specs=in_specs, out_specs=out_specs, check_vma=False)
```

```python
import jax
import jax.numpy as jnp
from jax import lax
from jax.experimental import pallas as pl
from jax.experimental.pallas import tpu as pltpu
from jax.sharding import PartitionSpec as P

MESH = pl.DeviceIdType.MESH
PEERS = 16
HALF = 8
ROWS, COLS = 400, 256
GROUPS = ROWS // 8
RAW = 16
EARLY = 64
FIRST = RAW + EARLY
REST = ROWS - FIRST
FAR = [(1, dy, dc) for dy in (2, 1, 3, 0) for dc in (0, 1)]
NEAR = [(0, dy, dc) for dy in (2, 1, 3, 0) for dc in (0, 1) if (dy, dc) != (0, 0)]
OFFSETS = FAR + NEAR
BACK = [OFFSETS.index((dz, -dy % 4, dc)) for dz, dy, dc in OFFSETS]


def kernel(
    x_ref, w_ref, g_ref, o_ref, sc_ref, rt_ref,
    xbuf, send, raw, early_mine, early_all, early_out, early_in, part_mine, part_all, half_out, half_in, full_all,
    wbuf, rb,
    load_sem, in_sem, here_sem,
    early_s, early_r, part_s, part_r, ez_s, ez_r, hz_s, hz_r, full_s, full_r,
    raw_s, raw_r, da_s, da_r, db_s, db_r, z_s, z_r, xy_s, xy_r, co_s, co_r,
):
    e, s = lax.axis_index("expert"), lax.axis_index("shard")
    zl, xx = e // 4, e % 4
    zh, yy, cc = s // 8, (s // 2) % 4, s % 2
    zz = zh * 4 + zl
    u = s % 8

    def partner(k):
        dz, dy, dc = OFFSETS[k]
        return ((zh + dz) % 2) * 8 + ((yy + dy) % 4) * 2 + (cc + dc) % 2

    def on_line(k):
        z = (zz + k) % 8
        return {"expert": (z % 4) * 4 + xx, "shard": (z // 4) * 8 + yy * 2 + cc}

    def on_plane(k):
        x, y = (xx + k // 4) % 4, (yy + k % 4) % 4
        return {"expert": zl * 4 + x, "shard": zh * 8 + y * 2 + cc}

    near = range(len(FAR), PEERS - 1)
    across = {"shard": (s + 8) % 16}

    barrier = pltpu.get_barrier_semaphore()
    greeted = [on_line(k) for k in (4, 3, 5, 2, 6, 1, 7)]
    greeted += [on_plane(k) for k in range(4, 16)]
    greeted += [{"shard": partner(k)} for k in near]
    for device in greeted:
        pl.semaphore_signal(barrier, inc=1, device_id=device, device_id_type=MESH)

    def load(d):
        return pltpu.make_async_copy(x_ref.at[pl.ds(d * ROWS, ROWS)], xbuf.at[d], load_sem.at[d])

    def start_load(d, carry):
        load(d).start()
        return carry

    lax.fori_loop(0, PEERS, start_load, 0)
    small = [
        pltpu.make_async_copy(w_ref, wbuf.at[0], in_sem.at[0]),
        pltpu.make_async_copy(g_ref, wbuf.at[1], in_sem.at[1]),
    ]
    for c in small:
        c.start()
    for c in small:
        c.wait()
    rb[xx, yy, cc, zz] = (wbuf[0] * wbuf[1]).astype(jnp.bfloat16).astype(jnp.float32)

    lane = lax.broadcasted_iota(jnp.int32, (8, 128), 1)

    def maxima(v, early):
        part = jnp.zeros((8, 128), jnp.float32)
        for h in range(2):
            d = h * HALF + v
            load(d).wait()
            for g in range(GROUPS):
                a = jnp.abs(xbuf[d, 8 * g : 8 * g + 8, :])
                top = jnp.max(jnp.maximum(a[:, :128], a[:, 128:]), axis=1, keepdims=True)
                part = jnp.where(lane == h * 64 + g, top, part)
                if RAW <= 8 * g < FIRST:
                    early = jnp.where(lane == d * (EARLY // 8) + g - RAW // 8, top, early)
        part_mine[v] = part
        return early

    early_mine[...] = lax.fori_loop(0, HALF, maxima, jnp.zeros((8, 128), jnp.float32))
    early_all[u] = early_mine[...]
    part_all[u] = part_mine[u]

    pl.semaphore_wait(barrier, len(greeted))

    started, arrived = [], set()

    def remote(src, dst, ss, rs, device):
        c = pltpu.make_async_remote_copy(
            src_ref=src, dst_ref=dst, send_sem=ss, recv_sem=rs, device_id=device, device_id_type=MESH
        )
        c.start()
        started.append(c)
        return c

    def arrive(copies):
        for c in copies:
            c.wait_recv()
            arrived.add(id(c))

    def drain():
        for c in started:
            if id(c) not in arrived:
                c.wait_recv()
            c.wait_send()

    for k in near:
        pl.semaphore_signal(here_sem, inc=1, device_id={"shard": partner(k)}, device_id_type=MESH)
    early = [
        remote(early_mine, early_all.at[u], early_s.at[i], early_r.at[i], {"shard": partner(k)})
        for i, k in enumerate(near)
    ]
    part = [
        remote(part_mine.at[partner(k) % 8], part_all.at[u], part_s.at[i], part_r.at[i], {"shard": partner(k)})
        for i, k in enumerate(near)
    ]
    line = [
        remote(rb.at[xx, yy, cc, zz], rb.at[xx, yy, cc, zz], z_s.at[k], z_r.at[k], on_line(k)) for k in range(1, 8)
    ]
    pl.semaphore_wait(here_sem, len(near))
    rawc = []
    for k in range(PEERS - 1):
        d = partner(k)
        rawc.append(remote(xbuf.at[d, pl.ds(0, RAW)], raw.at[s], raw_s.at[k], raw_r.at[k], {"shard": d}))

    arrive(early)
    early_out[...] = jnp.max(early_all[...], axis=0)
    arrive(part)
    half_out[...] = jnp.max(part_all[...], axis=0)
    ez = remote(early_out, early_in, ez_s.at[0], ez_r.at[0], across)
    hz = remote(half_out, half_in, hz_s.at[0], hz_r.at[0], across)
    arrive([ez])
    inverse_early = 1.0 / jnp.maximum(early_out[...], early_in[...])
    arrive([hz])
    full_all[u] = jnp.maximum(half_out[...], half_in[...])
    full = [
        remote(full_all.at[u], full_all.at[u], full_s.at[i], full_r.at[i], {"shard": partner(k)})
        for i, k in enumerate(near)
    ]

    def early_rows(d):
        for j in range(EARLY // 16):
            tops = []
            for h in range(2):
                at = d * (EARLY // 8) + 2 * j + h
                tops.append(jnp.sum(jnp.where(lane == at, inverse_early, 0.0), axis=1, keepdims=True))
            lo = RAW + 16 * j
            send[d, lo : lo + 16, :] = (xbuf[d, lo : lo + 16, :] * jnp.concatenate(tops, axis=0)).astype(jnp.bfloat16)

    columns = pl.ds(pl.multiple_of(s * COLS, COLS), COLS)

    def send_rows(lo, count, ss, rs, k):
        d = partner(k)
        return remote(
            send.at[d, pl.ds(lo, count)], o_ref.at[pl.ds(lo, count), columns], ss.at[k], rs.at[k], {"shard": d}
        )

    for k in range(PEERS - 1):
        early_rows(partner(k))
        if k:
            send_rows(RAW, EARLY, da_s, da_r, k - 1)
    send_rows(RAW, EARLY, da_s, da_r, PEERS - 2)


    def inverse_of(h, tile):
        tile = jnp.where(lane % 64 < GROUPS, tile, 1.0)
        tile = 1.0 / tile
        return jnp.where(h == 0, tile, pltpu.roll(tile, 64, 1))

    def tops_of(inverse, j):
        return jnp.concatenate([inverse[:, 2 * j : 2 * j + 1], inverse[:, 2 * j + 1 : 2 * j + 2]], axis=0)

    def rest_rows(d):
        inverse = inverse_of(d // 8, full_all[d % 8])
        for j in range(FIRST // 16, ROWS // 16):
            send[d, 16 * j : 16 * j + 16, :] = (xbuf[d, 16 * j : 16 * j + 16, :] * tops_of(inverse, j)).astype(
                jnp.bfloat16
            )

    arrive(full)
    for k in range(PEERS - 1):
        rest_rows(partner(k))
        if k:
            send_rows(FIRST, REST, db_s, db_r, k - 1)
    send_rows(FIRST, REST, db_s, db_r, PEERS - 2)

    arrive(line)
    plane = [
        remote(rb.at[xx, yy, cc], rb.at[xx, yy, cc], xy_s.at[k], xy_r.at[k], on_plane(k)) for k in range(1, 16)
    ]

    mine = full_all[u]
    inverse_mine = inverse_of(zh, mine)
    for j in range(ROWS // 16):
        o_ref[16 * j : 16 * j + 16, columns] = (xbuf[s, 16 * j : 16 * j + 16, :] * tops_of(inverse_mine, j)).astype(
            jnp.bfloat16
        )
    arrive(rawc)
    for k in range(PEERS - 1):
        d = partner(k)
        for j in range(RAW // 16):
            o_ref[16 * j : 16 * j + 16, pl.ds(pl.multiple_of(d * COLS, COLS), COLS)] = (
                raw[d, 16 * j : 16 * j + 16, :] * tops_of(inverse_mine, j)
            ).astype(jnp.bfloat16)

    mine = jnp.where(zh == 0, mine, pltpu.roll(mine, 64, 1))
    sub = lax.broadcasted_iota(jnp.int32, (8, 128), 0)
    for b in range(pl.cdiv(ROWS, 128)):
        row = jnp.zeros((8, 128), jnp.float32)
        for g in range(16 * b, min(16 * b + 16, GROUPS)):
            here = (lane // 8 == g - 16 * b) & (sub == lane % 8)
            row = jnp.where(here, jnp.broadcast_to(mine[:, g : g + 1], (8, 128)), row)
        width = min(128, ROWS - 128 * b)
        sc_ref[:, 128 * b : 128 * b + width] = jnp.max(row, axis=0, keepdims=True)[:, :width]

    arrive(plane)
    other = remote(
        rb.at[:, :, cc], rb.at[:, :, cc], co_s.at[0], co_r.at[0],
        {"shard": zh * 8 + yy * 2 + 1 - cc},
    )
    arrive([other])

    def router_columns(t, carry):
        h, y, c = t // 8, (t // 2) % 4, t % 2
        rows = [rb[r % 4, y, c, h * 4 + r // 4] for r in range(16)]
        rt_ref[:, pl.ds(pl.multiple_of(t * COLS, COLS), COLS)] = jnp.concatenate(rows, axis=0).astype(jnp.bfloat16)
        return carry

    lax.fori_loop(0, PEERS, router_columns, 0)

    drain()


def finish(o_ref, sc_ref, rt_ref, out_o, out_sc, out_rt, sem):
    copies = [
        pltpu.make_async_copy(o_ref, out_o, sem.at[0]),
        pltpu.make_async_copy(sc_ref, out_sc, sem.at[1]),
        pltpu.make_async_copy(rt_ref, out_rt, sem.at[2]),
    ]
    for c in copies:
        c.start()
    for c in copies:
        c.wait()


def per_device(train_down, router_weight, router_gain):
    keep = lambda a: pltpu.with_memory_space_constraint(a, pltpu.HBM)
    x = keep(train_down[0])
    w = keep(router_weight.reshape(1, COLS))
    g = keep(router_gain.reshape(1, COLS))
    f32, bf16 = jnp.float32, jnp.bfloat16
    dma = pltpu.SemaphoreType.DMA
    pairs = lambda n: [dma((n,)), dma((n,))]
    tile = lambda *n: pltpu.VMEM((*n, 8, 128), f32)
    n, m = PEERS - 1, HALF - 1
    hbm = pl.BlockSpec(memory_space=pltpu.HBM)
    vmem = pl.BlockSpec(memory_space=pltpu.VMEM)
    o, sc, rt = pl.pallas_call(
        kernel,
        out_shape=(
            pltpu.VMEM((ROWS, PEERS * COLS), bf16),
            pltpu.VMEM((1, ROWS), f32),
            pltpu.VMEM((PEERS, PEERS * COLS), bf16),
        ),
        in_specs=[hbm] * 3,
        out_specs=(vmem,) * 3,
        scratch_shapes=[
            pltpu.VMEM((PEERS, ROWS, COLS), f32),
            pltpu.VMEM((PEERS, ROWS, COLS), bf16),
            pltpu.VMEM((PEERS, RAW, COLS), f32),
            tile(), tile(HALF), tile(), tile(),
            tile(HALF), tile(HALF), tile(), tile(), tile(HALF),
            pltpu.VMEM((2, 1, COLS), f32),
            pltpu.VMEM((4, 4, 2, 8, 1, COLS), f32),
            dma((PEERS,)), dma((2,)), pltpu.SemaphoreType.REGULAR,
            *pairs(m), *pairs(m), *pairs(1), *pairs(1), *pairs(m),
            *pairs(n), *pairs(n), *pairs(n),
            *pairs(8), *pairs(16), *pairs(1),
        ],
        compiler_params=pltpu.CompilerParams(
            collective_id=0, has_side_effects=True, vmem_limit_bytes=40 * 2**20
        ),
        name="exchange",
    )(x, w, g)
    inside = lambda a: pltpu.with_memory_space_constraint(a, pltpu.VMEM)
    ready, scale, router = pl.pallas_call(
        finish,
        out_shape=(
            jax.ShapeDtypeStruct((ROWS, PEERS * COLS), bf16),
            jax.ShapeDtypeStruct((1, ROWS), f32),
            jax.ShapeDtypeStruct((PEERS, PEERS * COLS), bf16),
        ),
        in_specs=[vmem] * 3,
        out_specs=(hbm,) * 3,
        scratch_shapes=[dma((3,))],
        name="finish",
    )(inside(o), inside(sc), inside(rt))
    return ready[None], scale, router.T


def solution(mesh):
    in_specs = (P("expert", None, "shard"), P("shard", "expert"), P("shard"))
    out_specs = (P("expert", "shard", None), P("expert", "shard"), P())
    return jax.shard_map(per_device, mesh=mesh, in_specs=in_specs, out_specs=out_specs, check_vma=False)
```

```python
import jax
import jax.numpy as jnp
from jax import lax
from jax.experimental import pallas as pl
from jax.experimental.pallas import tpu as pltpu
from jax.sharding import PartitionSpec as P

MESH = pl.DeviceIdType.MESH
PEERS = 16
HALF = 8
ROWS, COLS = 400, 256
GROUPS = ROWS // 8
BLOCK = 64
STEPS = 2
EARLY = BLOCK * STEPS
REST = ROWS - EARLY
CUTS = 5
LOAD = 4
PART, HZ, FULL, DATA_REST, LINE, PLANE, OTHER = range(7)
EARLIES = range(7, 7 + STEPS)
DATA_EARLY = range(7 + STEPS, 7 + 2 * STEPS)
KINDS = 7 + 2 * STEPS
FAR = [(1, dy, dc) for dy in (2, 1, 3, 0) for dc in (0, 1)]
NEAR = [(0, dy, dc) for dy in (2, 1, 3, 0) for dc in (0, 1) if (dy, dc) != (0, 0)]
OFFSETS = FAR + NEAR


def kernel(
    x_ref, w_ref, g_ref, o_ref, sc_ref, rt_ref,
    xbuf, send, early_mine, early_all, part_mine, part_all, half_out, half_in, full_all,
    wbuf, rb,
    load_sem, in_sem, sent, got,
):
    e, s = lax.axis_index("expert"), lax.axis_index("shard")
    zl, xx = e // 4, e % 4
    zh, yy, cc = s // 8, (s // 2) % 4, s % 2
    zz = zh * 4 + zl
    u = s % 8

    def partner(k):
        dz, dy, dc = OFFSETS[k]
        return ((zh + dz) % 2) * 8 + ((yy + dy) % 4) * 2 + (cc + dc) % 2

    def on_line(k):
        z = (zz + k) % 8
        return {"expert": (z % 4) * 4 + xx, "shard": (z // 4) * 8 + yy * 2 + cc}

    def on_plane(k):
        x, y = (xx + k // 4) % 4, (yy + k % 4) % 4
        return {"expert": zl * 4 + x, "shard": zh * 8 + y * 2 + cc}

    near = range(len(FAR), PEERS - 1)
    across = {"shard": (s + 8) % 16}

    barrier = pltpu.get_barrier_semaphore()
    greeted = [{"shard": partner(k)} for k in range(PEERS - 1)]
    greeted += [on_line(k) for k in (3, 5, 2, 6, 1, 7)]
    greeted += [on_plane(k) for k in range(4, 16)]
    for device in greeted:
        pl.semaphore_signal(barrier, inc=1, device_id=device, device_id_type=MESH)

    def load(q):
        if q < STEPS:
            here = (slice(None), pl.ds(q * BLOCK, BLOCK))
        else:
            here = (pl.ds((q - STEPS) * LOAD, LOAD), pl.ds(EARLY, REST))
        return pltpu.make_async_copy(x_ref.at[here], xbuf.at[here], load_sem.at[q])

    loads = [load(q) for q in range(STEPS + PEERS // LOAD)]
    for c in loads:
        c.start()
    pltpu.make_async_copy(w_ref, wbuf.at[0], in_sem).start()
    pltpu.make_async_copy(g_ref, wbuf.at[1], in_sem).start()

    lane = lax.broadcasted_iota(jnp.int32, (8, 128), 1)

    def top_of(d, g):
        a = jnp.abs(xbuf[d, 8 * g : 8 * g + 8, :])
        return jnp.max(jnp.maximum(a[:, :128], a[:, 128:]), axis=1, keepdims=True)

    def early_maxima(t):
        def one(d, early):
            h, v = d // HALF, d % HALF
            part = part_mine[v]
            for g in range(BLOCK // 8):
                top = top_of(d, t * (BLOCK // 8) + g)
                part = jnp.where(lane == h * 64 + t * (BLOCK // 8) + g, top, part)
                early = jnp.where(lane == d * (BLOCK // 8) + g, top, early)
            part_mine[v] = part
            return early

        loads[t].wait()
        early_mine[t] = lax.fori_loop(0, PEERS, one, jnp.zeros((8, 128), jnp.float32))
        early_all[t, s] = early_mine[t]

    def rest_maxima(d, carry):
        h, v = d // HALF, d % HALF
        part = part_mine[v]
        for g in range(EARLY // 8, GROUPS):
            part = jnp.where(lane == h * 64 + g, top_of(d, g), part)
        part_mine[v] = part
        return carry

    part_mine[...] = jnp.zeros((HALF, 8, 128), jnp.float32)
    early_maxima(0)

    pl.semaphore_wait(barrier, len(greeted))

    def remote(src, dst, kind, device):
        pltpu.make_async_remote_copy(
            src_ref=src, dst_ref=dst, send_sem=sent.at[kind], recv_sem=got.at[kind],
            device_id=device, device_id_type=MESH,
        ).start()

    amount = {
        PART: part_all.at[pl.ds(0, HALF - 1)],
        HZ: half_in,
        FULL: full_all.at[pl.ds(0, HALF - 1)],
        DATA_REST: send.at[pl.ds(0, PEERS - 1), pl.ds(0, REST)],
        LINE: rb.at[0, 0, 0, pl.ds(0, 7)],
        PLANE: xbuf.at[0, pl.ds(0, 15 * 8)],
        OTHER: xbuf.at[0, pl.ds(0, 16 * 8)],
    }

    for t in range(STEPS):
        amount[EARLIES[t]] = early_all.at[t, pl.ds(0, PEERS - 1)]
        amount[DATA_EARLY[t]] = send.at[pl.ds(0, PEERS - 1), pl.ds(0, BLOCK)]

    def arrive(kind):
        pltpu.make_async_copy(amount[kind], amount[kind], got.at[kind]).wait()

    def leave(kind):
        pltpu.make_async_copy(amount[kind], amount[kind], sent.at[kind]).wait()

    for t in range(STEPS):
        if t:
            early_maxima(t)
        for k in range(PEERS - 1):
            remote(early_mine.at[t], early_all.at[t, s], EARLIES[t], {"shard": partner(k)})

    for q in range(PEERS // LOAD):
        loads[STEPS + q].wait()
        lax.fori_loop(q * LOAD, q * LOAD + LOAD, rest_maxima, 0)
    part_all[u] = part_mine[u]
    for k in near:
        remote(part_mine.at[partner(k) % 8], part_all.at[u], PART, {"shard": partner(k)})
    pltpu.make_async_copy(wbuf, wbuf, in_sem).wait()
    rb[xx, yy, cc, zz] = (wbuf[0] * wbuf[1]).astype(jnp.bfloat16).astype(jnp.float32)
    for k in range(1, 8):
        remote(rb.at[xx, yy, cc, zz], rb.at[xx, yy, cc, zz], LINE, on_line(k))

    def early_rows(t, d, inverse):
        for j in range(BLOCK // 16):
            tops = []
            for h in range(2):
                at = d * (BLOCK // 8) + 2 * j + h
                tops.append(jnp.sum(jnp.where(lane == at, inverse, 0.0), axis=1, keepdims=True))
            lo = t * BLOCK + 16 * j
            send[d, lo : lo + 16, :] = (xbuf[d, lo : lo + 16, :] * jnp.concatenate(tops, axis=0)).astype(jnp.bfloat16)

    columns = pl.ds(pl.multiple_of(s * COLS, COLS), COLS)

    def send_rows(lo, count, kind, k):
        d = partner(k)
        remote(send.at[d, pl.ds(lo, count)], o_ref.at[pl.ds(lo, count), columns], kind, {"shard": d})

    for t in range(STEPS):
        arrive(EARLIES[t])
        if t == 0:
            arrive(PART)
            half_out[...] = jnp.max(part_all[...], axis=0)
            remote(half_out, half_in, HZ, across)
        inverse = 1.0 / jnp.max(early_all[t], axis=0)
        for k in range(PEERS):
            if k < PEERS - 1:
                early_rows(t, partner(k), inverse)
            if k:
                send_rows(t * BLOCK, BLOCK, DATA_EARLY[t], k - 1)

    arrive(HZ)
    full_all[u] = jnp.maximum(half_out[...], half_in[...])
    for k in near:
        remote(full_all.at[u], full_all.at[u], FULL, {"shard": partner(k)})

    def inverse_of(h, tile):
        tile = jnp.where(lane % 64 < GROUPS, tile, 1.0)
        tile = 1.0 / tile
        return jnp.where(h == 0, tile, pltpu.roll(tile, 64, 1))

    def tops_of(inverse, j):
        return jnp.concatenate([inverse[:, 2 * j : 2 * j + 1], inverse[:, 2 * j + 1 : 2 * j + 2]], axis=0)

    def rest_rows(d):
        inverse = inverse_of(d // 8, full_all[d % 8])
        for j in range(EARLY // 16, ROWS // 16):
            send[d, 16 * j : 16 * j + 16, :] = (xbuf[d, 16 * j : 16 * j + 16, :] * tops_of(inverse, j)).astype(
                jnp.bfloat16
            )

    arrive(FULL)
    for k in range(PEERS):
        if k < PEERS - 1:
            rest_rows(partner(k))
        if k:
            send_rows(EARLY, REST, DATA_REST, k - 1)

    arrive(LINE)
    for k in range(1, 16):
        remote(rb.at[xx, yy, cc], rb.at[xx, yy, cc], PLANE, on_plane(k))

    mine = full_all[u]
    inverse_mine = inverse_of(zh, mine)
    for j in range(ROWS // 16):
        o_ref[16 * j : 16 * j + 16, columns] = (xbuf[s, 16 * j : 16 * j + 16, :] * tops_of(inverse_mine, j)).astype(
            jnp.bfloat16
        )
    mine = jnp.where(zh == 0, mine, pltpu.roll(mine, 64, 1))
    sub = lax.broadcasted_iota(jnp.int32, (8, 128), 0)
    for b in range(pl.cdiv(ROWS, 128)):
        row = jnp.zeros((8, 128), jnp.float32)
        for g in range(16 * b, min(16 * b + 16, GROUPS)):
            here = (lane // 8 == g - 16 * b) & (sub == lane % 8)
            row = jnp.where(here, jnp.broadcast_to(mine[:, g : g + 1], (8, 128)), row)
        width = min(128, ROWS - 128 * b)
        sc_ref[:, 128 * b : 128 * b + width] = jnp.max(row, axis=0, keepdims=True)[:, :width]

    arrive(PLANE)
    remote(rb.at[:, :, cc], rb.at[:, :, cc], OTHER, {"shard": zh * 8 + yy * 2 + 1 - cc})
    arrive(OTHER)

    def router_columns(t, carry):
        h, y, c = t // 8, (t // 2) % 4, t % 2
        rows = [rb[r % 4, y, c, h * 4 + r // 4] for r in range(16)]
        rt_ref[:, pl.ds(pl.multiple_of(t * COLS, COLS), COLS)] = jnp.concatenate(rows, axis=0).astype(jnp.bfloat16)
        return carry

    lax.fori_loop(0, PEERS, router_columns, 0)

    for kind in (*DATA_EARLY, DATA_REST):
        arrive(kind)
    for kind in range(KINDS):
        leave(kind)


def finish(o_ref, sc_ref, rt_ref, out_o, out_sc, out_rt, sem):
    copies = [
        pltpu.make_async_copy(sc_ref, out_sc, sem.at[0]),
        pltpu.make_async_copy(rt_ref, out_rt, sem.at[1]),
    ]
    for k in range(CUTS):
        rows = pl.ds(k * (ROWS // CUTS), ROWS // CUTS)
        copies.append(pltpu.make_async_copy(o_ref.at[rows], out_o.at[rows], sem.at[2 + k]))
    for c in copies:
        c.start()
    for c in copies:
        c.wait()


def per_device(train_down, router_weight, router_gain):
    keep = lambda a: pltpu.with_memory_space_constraint(a, pltpu.HBM)
    x = keep(train_down.reshape(PEERS, ROWS, COLS))
    w = keep(router_weight.reshape(1, COLS))
    g = keep(router_gain.reshape(1, COLS))
    f32, bf16 = jnp.float32, jnp.bfloat16
    dma = pltpu.SemaphoreType.DMA
    tile = lambda *n: pltpu.VMEM((*n, 8, 128), f32)
    hbm = pl.BlockSpec(memory_space=pltpu.HBM)
    vmem = pl.BlockSpec(memory_space=pltpu.VMEM)
    o, sc, rt = pl.pallas_call(
        kernel,
        out_shape=(
            pltpu.VMEM((ROWS, PEERS * COLS), bf16),
            pltpu.VMEM((1, ROWS), f32),
            pltpu.VMEM((PEERS, PEERS * COLS), bf16),
        ),
        in_specs=[hbm] * 3,
        out_specs=(vmem,) * 3,
        scratch_shapes=[
            pltpu.VMEM((PEERS, ROWS, COLS), f32),
            pltpu.VMEM((PEERS, ROWS, COLS), bf16),
            tile(STEPS), tile(STEPS, PEERS),
            tile(HALF), tile(HALF), tile(), tile(), tile(HALF),
            pltpu.VMEM((2, 1, COLS), f32),
            pltpu.VMEM((4, 4, 2, 8, 1, COLS), f32),
            dma((STEPS + PEERS // LOAD,)), dma, dma((KINDS,)), dma((KINDS,)),
        ],
        compiler_params=pltpu.CompilerParams(
            collective_id=0, has_side_effects=True, vmem_limit_bytes=40 * 2**20
        ),
        name="exchange",
    )(x, w, g)
    inside = lambda a: pltpu.with_memory_space_constraint(a, pltpu.VMEM)
    ready, scale, router = pl.pallas_call(
        finish,
        out_shape=(
            jax.ShapeDtypeStruct((ROWS, PEERS * COLS), bf16),
            jax.ShapeDtypeStruct((1, ROWS), f32),
            jax.ShapeDtypeStruct((PEERS, PEERS * COLS), bf16),
        ),
        in_specs=[vmem] * 3,
        out_specs=(hbm,) * 3,
        scratch_shapes=[dma((2 + CUTS,))],
        name="finish",
    )(inside(o), inside(sc), inside(rt))
    return ready[None], scale, router.T


def solution(mesh):
    in_specs = (P("expert", None, "shard"), P("shard", "expert"), P("shard"))
    out_specs = (P("expert", "shard", None), P("expert", "shard"), P())
    return jax.shard_map(per_device, mesh=mesh, in_specs=in_specs, out_specs=out_specs, check_vma=False)
```

```python
import jax
import jax.numpy as jnp
from jax import lax
from jax.experimental import pallas as pl
from jax.experimental.pallas import tpu as pltpu
from jax.sharding import PartitionSpec as P

MESH = pl.DeviceIdType.MESH
PEERS = 16
HALF = 8
ROWS, COLS = 400, 256
GROUPS = ROWS // 8
BLOCK = 64
STEPS = 1
EARLY = BLOCK * STEPS
REST = ROWS - EARLY
CUTS = 5
LOAD = 4
PART, HZ, FULL, DATA_REST, OVER_ZH, OVER_ZL, OVER_X, OVER_Y, OVER_CORE = range(9)
EARLIES = range(9, 9 + STEPS)
DATA_EARLY = range(9 + STEPS, 9 + 2 * STEPS)
KINDS = 9 + 2 * STEPS
FAR = [(1, dy, dc) for dy in (2, 1, 3, 0) for dc in (0, 1)]
NEAR = [(0, dy, dc) for dy in (2, 1, 3, 0) for dc in (0, 1) if (dy, dc) != (0, 0)]
OFFSETS = FAR + NEAR


def kernel(
    x_ref, w_ref, g_ref, o_ref, sc_ref, rt_ref,
    xbuf, send, early_mine, early_all, part_mine, part_all, half_out, half_in, full_all,
    wbuf, rb,
    load_sem, in_sem, sent, got,
):
    e, s = lax.axis_index("expert"), lax.axis_index("shard")
    zl, xx = e // 4, e % 4
    zh, yy, cc = s // 8, (s // 2) % 4, s % 2
    u = s % 8

    def partner(k):
        dz, dy, dc = OFFSETS[k]
        return ((zh + dz) % 2) * 8 + ((yy + dy) % 4) * 2 + (cc + dc) % 2

    along_zl = [{"expert": (zl + k) % 4 * 4 + xx, "shard": s} for k in (2, 1, 3)]
    along_x = [{"expert": zl * 4 + (xx + k) % 4, "shard": s} for k in (2, 1, 3)]
    along_y = [{"shard": zh * 8 + (yy + k) % 4 * 2 + cc} for k in (2, 1, 3)]

    near = range(len(FAR), PEERS - 1)
    across = {"shard": (s + 8) % 16}

    def load(q):
        if q < STEPS:
            here = (slice(None), pl.ds(q * BLOCK, BLOCK))
        else:
            here = (pl.ds((q - STEPS) * LOAD, LOAD), pl.ds(EARLY, REST))
        return pltpu.make_async_copy(x_ref.at[here], xbuf.at[here], load_sem.at[q])

    loads = [load(q) for q in range(STEPS + PEERS // LOAD)]
    loads[0].start()

    barrier = pltpu.get_barrier_semaphore()
    greeted = [{"shard": partner(k)} for k in range(PEERS - 1)] + along_zl + along_x
    for device in greeted:
        pl.semaphore_signal(barrier, inc=1, device_id=device, device_id_type=MESH)

    for c in loads[1:]:
        c.start()
    pltpu.make_async_copy(w_ref, wbuf.at[0], in_sem).start()
    pltpu.make_async_copy(g_ref, wbuf.at[1], in_sem).start()

    lane = lax.broadcasted_iota(jnp.int32, (8, 128), 1)

    def top_of(d, g):
        a = jnp.abs(xbuf[d, 8 * g : 8 * g + 8, :])
        return jnp.max(jnp.maximum(a[:, :128], a[:, 128:]), axis=1, keepdims=True)

    def early_maxima(t):
        def one(d, early):
            h, v = d // HALF, d % HALF
            part = part_mine[v]
            for g in range(BLOCK // 8):
                top = top_of(d, t * (BLOCK // 8) + g)
                part = jnp.where(lane == h * 64 + t * (BLOCK // 8) + g, top, part)
                early = jnp.where(lane == d * (BLOCK // 8) + g, top, early)
            part_mine[v] = part
            return early

        loads[t].wait()
        early_mine[t] = lax.fori_loop(0, PEERS, one, jnp.zeros((8, 128), jnp.float32))
        early_all[t, s] = early_mine[t]

    def rest_maxima(d, carry):
        h, v = d // HALF, d % HALF
        part = part_mine[v]
        for g in range(EARLY // 8, GROUPS):
            part = jnp.where(lane == h * 64 + g, top_of(d, g), part)
        part_mine[v] = part
        return carry

    part_mine[...] = jnp.zeros((HALF, 8, 128), jnp.float32)
    for t in range(STEPS):
        early_maxima(t)
    for q in range(PEERS // LOAD):
        loads[STEPS + q].wait()
        lax.fori_loop(q * LOAD, q * LOAD + LOAD, rest_maxima, 0)
    part_all[u] = part_mine[u]
    pltpu.make_async_copy(wbuf, wbuf, in_sem).wait()
    rb[xx, yy, cc, zl, zh] = (wbuf[0] * wbuf[1]).astype(jnp.bfloat16).astype(jnp.float32)

    pl.semaphore_wait(barrier, len(greeted))

    def remote(src, dst, kind, device):
        pltpu.make_async_remote_copy(
            src_ref=src, dst_ref=dst, send_sem=sent.at[kind], recv_sem=got.at[kind],
            device_id=device, device_id_type=MESH,
        ).start()

    amount = {
        PART: part_all.at[pl.ds(0, HALF - 1)],
        HZ: half_in,
        FULL: full_all.at[pl.ds(0, HALF - 1)],
        DATA_REST: send.at[pl.ds(0, PEERS - 1), pl.ds(0, REST)],
        OVER_ZH: rb.at[0, 0, 0, 0, 0],
        OVER_ZL: rb.at[0, 0, 0, pl.ds(0, 3)],
        OVER_X: xbuf.at[0, pl.ds(0, 3 * 8)],
        OVER_Y: xbuf.at[0, pl.ds(0, 3 * 32)],
        OVER_CORE: xbuf.at[0, pl.ds(0, 128)],
    }

    for t in range(STEPS):
        amount[EARLIES[t]] = early_all.at[t, pl.ds(0, PEERS - 1)]
        amount[DATA_EARLY[t]] = send.at[pl.ds(0, PEERS - 1), pl.ds(0, BLOCK)]

    def arrive(kind):
        pltpu.make_async_copy(amount[kind], amount[kind], got.at[kind]).wait()

    def leave(kind):
        pltpu.make_async_copy(amount[kind], amount[kind], sent.at[kind]).wait()

    def send_tile(t, k):
        remote(early_mine.at[t], early_all.at[t, s], EARLIES[t], {"shard": partner(k)})

    for k in range(len(FAR)):
        send_tile(0, k)
    for k in near:
        remote(part_mine.at[partner(k) % 8], part_all.at[u], PART, {"shard": partner(k)})
    for k in near:
        send_tile(0, k)
    for t in range(1, STEPS):
        for k in range(PEERS - 1):
            send_tile(t, k)
    own = rb.at[xx, yy, cc, zl, zh]
    remote(own, own, OVER_ZH, across)

    def early_rows(t, d, inverse):
        for j in range(BLOCK // 16):
            tops = []
            for h in range(2):
                at = d * (BLOCK // 8) + 2 * j + h
                tops.append(jnp.sum(jnp.where(lane == at, inverse, 0.0), axis=1, keepdims=True))
            lo = t * BLOCK + 16 * j
            send[d, lo : lo + 16, :] = (xbuf[d, lo : lo + 16, :] * jnp.concatenate(tops, axis=0)).astype(jnp.bfloat16)

    columns = pl.ds(pl.multiple_of(s * COLS, COLS), COLS)

    def send_rows(lo, count, kind, k):
        d = partner(k)
        remote(send.at[d, pl.ds(lo, count)], o_ref.at[pl.ds(lo, count), columns], kind, {"shard": d})

    arrive(PART)
    half_out[...] = jnp.max(part_all[...], axis=0)
    remote(half_out, half_in, HZ, across)

    for t in range(STEPS):
        arrive(EARLIES[t])
        inverse = 1.0 / jnp.max(early_all[t], axis=0)
        for k in range(PEERS):
            if k < PEERS - 1:
                early_rows(t, partner(k), inverse)
            if k:
                send_rows(t * BLOCK, BLOCK, DATA_EARLY[t], k - 1)

    def pass_on(kind, part, devices):
        for device in devices:
            remote(part, part, kind, device)

    arrive(OVER_ZH)
    pass_on(OVER_ZL, rb.at[xx, yy, cc, zl], along_zl)

    arrive(HZ)
    full_all[u] = jnp.maximum(half_out[...], half_in[...])
    for k in near:
        remote(full_all.at[u], full_all.at[u], FULL, {"shard": partner(k)})

    def inverse_of(h, tile):
        tile = jnp.where(lane % 64 < GROUPS, tile, 1.0)
        tile = 1.0 / tile
        return jnp.where(h == 0, tile, pltpu.roll(tile, 64, 1))

    def tops_of(inverse, j):
        return jnp.concatenate([inverse[:, 2 * j : 2 * j + 1], inverse[:, 2 * j + 1 : 2 * j + 2]], axis=0)

    def rest_rows(d):
        inverse = inverse_of(d // 8, full_all[d % 8])
        for j in range(EARLY // 16, ROWS // 16):
            send[d, 16 * j : 16 * j + 16, :] = (xbuf[d, 16 * j : 16 * j + 16, :] * tops_of(inverse, j)).astype(
                jnp.bfloat16
            )

    arrive(FULL)
    for k in range(PEERS):
        if k < PEERS - 1:
            rest_rows(partner(k))
        if k:
            send_rows(EARLY, REST, DATA_REST, k - 1)

    arrive(OVER_ZL)
    pass_on(OVER_X, rb.at[xx, yy, cc], along_x)

    mine = full_all[u]
    inverse_mine = inverse_of(zh, mine)
    for j in range(ROWS // 16):
        o_ref[16 * j : 16 * j + 16, columns] = (xbuf[s, 16 * j : 16 * j + 16, :] * tops_of(inverse_mine, j)).astype(
            jnp.bfloat16
        )
    arrive(OVER_X)
    pass_on(OVER_Y, rb.at[:, yy, cc], along_y)

    mine = jnp.where(zh == 0, mine, pltpu.roll(mine, 64, 1))
    sub = lax.broadcasted_iota(jnp.int32, (8, 128), 0)
    for b in range(pl.cdiv(ROWS, 128)):
        row = jnp.zeros((8, 128), jnp.float32)
        for g in range(16 * b, min(16 * b + 16, GROUPS)):
            here = (lane // 8 == g - 16 * b) & (sub == lane % 8)
            row = jnp.where(here, jnp.broadcast_to(mine[:, g : g + 1], (8, 128)), row)
        width = min(128, ROWS - 128 * b)
        sc_ref[:, 128 * b : 128 * b + width] = jnp.max(row, axis=0, keepdims=True)[:, :width]

    arrive(OVER_Y)
    pass_on(OVER_CORE, rb.at[:, :, cc], [{"shard": zh * 8 + yy * 2 + 1 - cc}])
    arrive(OVER_CORE)

    def router_columns(t, carry):
        h, y, c = t // 8, (t // 2) % 4, t % 2
        rows = [rb[r % 4, y, c, r // 4, h] for r in range(16)]
        rt_ref[:, pl.ds(pl.multiple_of(t * COLS, COLS), COLS)] = jnp.concatenate(rows, axis=0).astype(jnp.bfloat16)
        return carry

    lax.fori_loop(0, PEERS, router_columns, 0)

    for kind in (*DATA_EARLY, DATA_REST):
        arrive(kind)
    for kind in range(KINDS):
        leave(kind)


def finish(o_ref, sc_ref, rt_ref, out_o, out_sc, out_rt, sem):
    copies = [
        pltpu.make_async_copy(sc_ref, out_sc, sem.at[0]),
        pltpu.make_async_copy(rt_ref, out_rt, sem.at[1]),
    ]
    for k in range(CUTS):
        rows = pl.ds(k * (ROWS // CUTS), ROWS // CUTS)
        copies.append(pltpu.make_async_copy(o_ref.at[rows], out_o.at[rows], sem.at[2 + k]))
    for c in copies:
        c.start()
    for c in copies:
        c.wait()


def per_device(train_down, router_weight, router_gain):
    keep = lambda a: pltpu.with_memory_space_constraint(a, pltpu.HBM)
    x = keep(train_down.reshape(PEERS, ROWS, COLS))
    w = keep(router_weight.reshape(1, COLS))
    g = keep(router_gain.reshape(1, COLS))
    f32, bf16 = jnp.float32, jnp.bfloat16
    dma = pltpu.SemaphoreType.DMA
    tile = lambda *n: pltpu.VMEM((*n, 8, 128), f32)
    hbm = pl.BlockSpec(memory_space=pltpu.HBM)
    vmem = pl.BlockSpec(memory_space=pltpu.VMEM)
    o, sc, rt = pl.pallas_call(
        kernel,
        out_shape=(
            pltpu.VMEM((ROWS, PEERS * COLS), bf16),
            pltpu.VMEM((1, ROWS), f32),
            pltpu.VMEM((PEERS, PEERS * COLS), bf16),
        ),
        in_specs=[hbm] * 3,
        out_specs=(vmem,) * 3,
        scratch_shapes=[
            pltpu.VMEM((PEERS, ROWS, COLS), f32),
            pltpu.VMEM((PEERS, ROWS, COLS), bf16),
            tile(STEPS), tile(STEPS, PEERS),
            tile(HALF), tile(HALF), tile(), tile(), tile(HALF),
            pltpu.VMEM((2, 1, COLS), f32),
            pltpu.VMEM((4, 4, 2, 4, 2, 1, COLS), f32),
            dma((STEPS + PEERS // LOAD,)), dma, dma((KINDS,)), dma((KINDS,)),
        ],
        compiler_params=pltpu.CompilerParams(
            collective_id=0, has_side_effects=True, vmem_limit_bytes=40 * 2**20
        ),
        name="exchange",
    )(x, w, g)
    inside = lambda a: pltpu.with_memory_space_constraint(a, pltpu.VMEM)
    ready, scale, router = pl.pallas_call(
        finish,
        out_shape=(
            jax.ShapeDtypeStruct((ROWS, PEERS * COLS), bf16),
            jax.ShapeDtypeStruct((1, ROWS), f32),
            jax.ShapeDtypeStruct((PEERS, PEERS * COLS), bf16),
        ),
        in_specs=[vmem] * 3,
        out_specs=(hbm,) * 3,
        scratch_shapes=[dma((2 + CUTS,))],
        name="finish",
    )(inside(o), inside(sc), inside(rt))
    return ready[None], scale, router.T


def solution(mesh):
    in_specs = (P("expert", None, "shard"), P("shard", "expert"), P("shard"))
    out_specs = (P("expert", "shard", None), P("expert", "shard"), P())
    return jax.shard_map(per_device, mesh=mesh, in_specs=in_specs, out_specs=out_specs, check_vma=False)
```

```python
import jax
import jax.numpy as jnp
from jax import lax
from jax.experimental import pallas as pl
from jax.experimental.pallas import tpu as pltpu
from jax.sharding import PartitionSpec as P

MESH = pl.DeviceIdType.MESH
PEERS = 16
HALF = 8
ROWS, COLS = 400, 256
GROUPS = ROWS // 8
BLOCK = 64
STEPS = 1
EARLY = BLOCK * STEPS
REST = ROWS - EARLY
CUTS = 2
LOAD = 4
PART, HZ, FULL, DATA_REST, OVER_ZH, OVER_ZL, OVER_X, OVER_Y, OVER_CORE = range(9)
EARLIES = range(9, 9 + STEPS)
DATA_EARLY = range(9 + STEPS, 9 + 2 * STEPS)
KINDS = 9 + 2 * STEPS
FAR = [(1, dy, dc) for dy in (2, 1, 3, 0) for dc in (0, 1)]
NEAR = [(0, dy, dc) for dy in (2, 1, 3, 0) for dc in (0, 1) if (dy, dc) != (0, 0)]
OFFSETS = FAR + NEAR


def kernel(
    x_ref, w_ref, g_ref, o_ref, sc_ref, rt_ref,
    xbuf, send, early_mine, early_all, part_mine, part_all, half_out, half_in, full_all,
    wbuf, rb,
    load_sem, in_sem, sent, got,
):
    e, s = lax.axis_index("expert"), lax.axis_index("shard")
    zl, xx = e // 4, e % 4
    zh, yy, cc = s // 8, (s // 2) % 4, s % 2
    u = s % 8

    def partner(k):
        dz, dy, dc = OFFSETS[k]
        return ((zh + dz) % 2) * 8 + ((yy + dy * (1 + 2 * cc)) % 4) * 2 + (cc + dc) % 2

    along_zl = [{"expert": (zl + k) % 4 * 4 + xx, "shard": s} for k in (2, 1, 3)]
    along_x = [{"expert": zl * 4 + (xx + k) % 4, "shard": s} for k in (2, 1, 3)]
    along_y = [{"shard": zh * 8 + (yy + k) % 4 * 2 + cc} for k in (2, 1, 3)]

    near = range(len(FAR), PEERS - 1)
    across = {"shard": (s + 8) % 16}

    def load(q):
        if q < STEPS:
            here = (slice(None), pl.ds(q * BLOCK, BLOCK))
        else:
            here = (pl.ds((q - STEPS) * LOAD, LOAD), pl.ds(EARLY, REST))
        return pltpu.make_async_copy(x_ref.at[here], xbuf.at[here], load_sem.at[q])

    loads = [load(q) for q in range(STEPS + PEERS // LOAD)]
    loads[0].start()

    barrier = pltpu.get_barrier_semaphore()
    greeted = [{"shard": partner(k)} for k in range(PEERS - 1)] + along_zl + along_x
    for i, device in enumerate(greeted):
        pl.semaphore_signal(barrier, inc=1, device_id=device, device_id_type=MESH)
        if i == len(FAR) - 1:
            for c in loads[1:]:
                c.start()
    pltpu.make_async_copy(w_ref, wbuf.at[0], in_sem).start()
    pltpu.make_async_copy(g_ref, wbuf.at[1], in_sem).start()

    lane = lax.broadcasted_iota(jnp.int32, (8, 128), 1)

    def top_of(d, g):
        a = jnp.abs(xbuf[d, 8 * g : 8 * g + 8, :])
        return jnp.max(jnp.maximum(a[:, :128], a[:, 128:]), axis=1, keepdims=True)

    def early_maxima(t):
        def one(d, early):
            h, v = d // HALF, d % HALF
            part = part_mine[v]
            for g in range(BLOCK // 8):
                top = top_of(d, t * (BLOCK // 8) + g)
                part = jnp.where(lane == h * 64 + t * (BLOCK // 8) + g, top, part)
                early = jnp.where(lane == d * (BLOCK // 8) + g, top, early)
            part_mine[v] = part
            return early

        loads[t].wait()
        early_mine[t] = lax.fori_loop(0, PEERS, one, jnp.zeros((8, 128), jnp.float32))
        early_all[t, s] = early_mine[t]

    def rest_maxima(d, carry):
        h, v = d // HALF, d % HALF
        part = part_mine[v]
        for g in range(EARLY // 8, GROUPS):
            part = jnp.where(lane == h * 64 + g, top_of(d, g), part)
        part_mine[v] = part
        return carry

    part_mine[...] = jnp.zeros((HALF, 8, 128), jnp.float32)
    for t in range(STEPS):
        early_maxima(t)
    for q in range(PEERS // LOAD):
        loads[STEPS + q].wait()
        lax.fori_loop(q * LOAD, q * LOAD + LOAD, rest_maxima, 0)
    part_all[u] = part_mine[u]
    pltpu.make_async_copy(wbuf, wbuf, in_sem).wait()
    rb[xx, yy, cc, zl, zh] = (wbuf[0] * wbuf[1]).astype(jnp.bfloat16).astype(jnp.float32)

    pl.semaphore_wait(barrier, len(greeted))

    def remote(src, dst, kind, device):
        pltpu.make_async_remote_copy(
            src_ref=src, dst_ref=dst, send_sem=sent.at[kind], recv_sem=got.at[kind],
            device_id=device, device_id_type=MESH,
        ).start()

    amount = {
        PART: part_all.at[pl.ds(0, HALF - 1)],
        HZ: half_in,
        FULL: full_all.at[pl.ds(0, HALF - 1)],
        DATA_REST: send.at[pl.ds(0, PEERS - 1), pl.ds(0, REST)],
        OVER_ZH: rb.at[0, 0, 0, 0, 0],
        OVER_ZL: rb.at[0, 0, 0, pl.ds(0, 3)],
        OVER_X: xbuf.at[0, pl.ds(0, 3 * 8)],
        OVER_Y: xbuf.at[0, pl.ds(0, 3 * 32)],
        OVER_CORE: xbuf.at[0, pl.ds(0, 128)],
    }

    for t in range(STEPS):
        amount[EARLIES[t]] = early_all.at[t, pl.ds(0, PEERS - 1)]
        amount[DATA_EARLY[t]] = send.at[pl.ds(0, PEERS - 1), pl.ds(0, BLOCK)]

    def arrive(kind):
        pltpu.make_async_copy(amount[kind], amount[kind], got.at[kind]).wait()

    def leave(kind):
        pltpu.make_async_copy(amount[kind], amount[kind], sent.at[kind]).wait()

    def send_tile(t, k):
        remote(early_mine.at[t], early_all.at[t, s], EARLIES[t], {"shard": partner(k)})

    for k in range(len(FAR)):
        send_tile(0, k)
    for k in near:
        send_tile(0, k)
    for k in near:
        remote(part_mine.at[partner(k) % 8], part_all.at[u], PART, {"shard": partner(k)})
    for t in range(1, STEPS):
        for k in range(PEERS - 1):
            send_tile(t, k)
    own = rb.at[xx, yy, cc, zl, zh]
    remote(own, own, OVER_ZH, across)

    def early_rows(t, d, inverse):
        for j in range(BLOCK // 16):
            tops = []
            for h in range(2):
                at = d * (BLOCK // 8) + 2 * j + h
                tops.append(jnp.sum(jnp.where(lane == at, inverse, 0.0), axis=1, keepdims=True))
            lo = t * BLOCK + 16 * j
            send[d, lo : lo + 16, :] = (xbuf[d, lo : lo + 16, :] * jnp.concatenate(tops, axis=0)).astype(jnp.bfloat16)

    columns = pl.ds(pl.multiple_of(s * COLS, COLS), COLS)

    def send_rows(lo, count, kind, k):
        d = partner(k)
        remote(send.at[d, pl.ds(lo, count)], o_ref.at[pl.ds(lo, count), columns], kind, {"shard": d})

    arrive(PART)
    half_out[...] = jnp.max(part_all[...], axis=0)
    remote(half_out, half_in, HZ, across)

    for t in range(STEPS):
        arrive(EARLIES[t])
        inverse = 1.0 / jnp.max(early_all[t], axis=0)
        for k in range(PEERS):
            if k < PEERS - 1:
                early_rows(t, partner(k), inverse)
            if k:
                send_rows(t * BLOCK, BLOCK, DATA_EARLY[t], k - 1)

    def pass_on(kind, part, devices):
        for device in devices:
            remote(part, part, kind, device)

    arrive(OVER_ZH)
    pass_on(OVER_ZL, rb.at[xx, yy, cc, zl], along_zl)

    arrive(HZ)
    full_all[u] = jnp.maximum(half_out[...], half_in[...])
    for k in near:
        remote(full_all.at[u], full_all.at[u], FULL, {"shard": partner(k)})

    def inverse_of(h, tile):
        tile = jnp.where(lane % 64 < GROUPS, tile, 1.0)
        tile = 1.0 / tile
        return jnp.where(h == 0, tile, pltpu.roll(tile, 64, 1))

    def tops_of(inverse, j):
        return jnp.concatenate([inverse[:, 2 * j : 2 * j + 1], inverse[:, 2 * j + 1 : 2 * j + 2]], axis=0)

    def rest_rows(d):
        inverse = inverse_of(d // 8, full_all[d % 8])
        for j in range(EARLY // 16, ROWS // 16):
            send[d, 16 * j : 16 * j + 16, :] = (xbuf[d, 16 * j : 16 * j + 16, :] * tops_of(inverse, j)).astype(
                jnp.bfloat16
            )

    arrive(FULL)
    for k in range(PEERS):
        if k < PEERS - 1:
            rest_rows(partner(k))
        if k:
            send_rows(EARLY, REST, DATA_REST, k - 1)

    arrive(OVER_ZL)
    pass_on(OVER_X, rb.at[xx, yy, cc], along_x)

    mine = full_all[u]
    inverse_mine = inverse_of(zh, mine)
    for j in range(ROWS // 16):
        o_ref[16 * j : 16 * j + 16, columns] = (xbuf[s, 16 * j : 16 * j + 16, :] * tops_of(inverse_mine, j)).astype(
            jnp.bfloat16
        )
    arrive(OVER_X)
    pass_on(OVER_Y, rb.at[:, yy, cc], along_y)

    mine = jnp.where(zh == 0, mine, pltpu.roll(mine, 64, 1))
    sub = lax.broadcasted_iota(jnp.int32, (8, 128), 0)
    for b in range(pl.cdiv(ROWS, 128)):
        row = jnp.zeros((8, 128), jnp.float32)
        for g in range(16 * b, min(16 * b + 16, GROUPS)):
            here = (lane // 8 == g - 16 * b) & (sub == lane % 8)
            row = jnp.where(here, jnp.broadcast_to(mine[:, g : g + 1], (8, 128)), row)
        width = min(128, ROWS - 128 * b)
        sc_ref[:, 128 * b : 128 * b + width] = jnp.max(row, axis=0, keepdims=True)[:, :width]

    arrive(OVER_Y)
    pass_on(OVER_CORE, rb.at[:, :, cc], [{"shard": zh * 8 + yy * 2 + 1 - cc}])
    arrive(OVER_CORE)

    def router_columns(t, carry):
        h, y, c = t // 8, (t // 2) % 4, t % 2
        rows = [rb[r % 4, y, c, r // 4, h] for r in range(16)]
        rt_ref[:, pl.ds(pl.multiple_of(t * COLS, COLS), COLS)] = jnp.concatenate(rows, axis=0).astype(jnp.bfloat16)
        return carry

    lax.fori_loop(0, PEERS, router_columns, 0)

    for kind in (*DATA_EARLY, DATA_REST):
        arrive(kind)
    for kind in range(KINDS):
        leave(kind)


def finish(o_ref, sc_ref, rt_ref, out_o, out_sc, out_rt, sem):
    copies = [
        pltpu.make_async_copy(sc_ref, out_sc, sem.at[0]),
        pltpu.make_async_copy(rt_ref, out_rt, sem.at[1]),
    ]
    for k in range(CUTS):
        rows = pl.ds(k * (ROWS // CUTS), ROWS // CUTS)
        copies.append(pltpu.make_async_copy(o_ref.at[rows], out_o.at[rows], sem.at[2 + k]))
    for c in copies:
        c.start()
    for c in copies:
        c.wait()


def per_device(train_down, router_weight, router_gain):
    keep = lambda a: pltpu.with_memory_space_constraint(a, pltpu.HBM)
    x = keep(train_down.reshape(PEERS, ROWS, COLS))
    w = keep(router_weight.reshape(1, COLS))
    g = keep(router_gain.reshape(1, COLS))
    f32, bf16 = jnp.float32, jnp.bfloat16
    dma = pltpu.SemaphoreType.DMA
    tile = lambda *n: pltpu.VMEM((*n, 8, 128), f32)
    hbm = pl.BlockSpec(memory_space=pltpu.HBM)
    vmem = pl.BlockSpec(memory_space=pltpu.VMEM)
    o, sc, rt = pl.pallas_call(
        kernel,
        out_shape=(
            pltpu.VMEM((ROWS, PEERS * COLS), bf16),
            pltpu.VMEM((1, ROWS), f32),
            pltpu.VMEM((PEERS, PEERS * COLS), bf16),
        ),
        in_specs=[hbm] * 3,
        out_specs=(vmem,) * 3,
        scratch_shapes=[
            pltpu.VMEM((PEERS, ROWS, COLS), f32),
            pltpu.VMEM((PEERS, ROWS, COLS), bf16),
            tile(STEPS), tile(STEPS, PEERS),
            tile(HALF), tile(HALF), tile(), tile(), tile(HALF),
            pltpu.VMEM((2, 1, COLS), f32),
            pltpu.VMEM((4, 4, 2, 4, 2, 1, COLS), f32),
            dma((STEPS + PEERS // LOAD,)), dma, dma((KINDS,)), dma((KINDS,)),
        ],
        compiler_params=pltpu.CompilerParams(
            collective_id=0, has_side_effects=True, vmem_limit_bytes=40 * 2**20
        ),
        name="exchange",
    )(x, w, g)
    inside = lambda a: pltpu.with_memory_space_constraint(a, pltpu.VMEM)
    ready, scale, router = pl.pallas_call(
        finish,
        out_shape=(
            jax.ShapeDtypeStruct((ROWS, PEERS * COLS), bf16),
            jax.ShapeDtypeStruct((1, ROWS), f32),
            jax.ShapeDtypeStruct((PEERS, PEERS * COLS), bf16),
        ),
        in_specs=[vmem] * 3,
        out_specs=(hbm,) * 3,
        scratch_shapes=[dma((2 + CUTS,))],
        name="finish",
    )(inside(o), inside(sc), inside(rt))
    return ready[None], scale, router.T


def solution(mesh):
    in_specs = (P("expert", None, "shard"), P("shard", "expert"), P("shard"))
    out_specs = (P("expert", "shard", None), P("expert", "shard"), P())
    return jax.shard_map(per_device, mesh=mesh, in_specs=in_specs, out_specs=out_specs, check_vma=False)
```
